32 devices in a mesh: batch: 1 (over z), row: 4 (over y), col: 8 (over x, core).
Axes of the slice: x: 4, y: 4, z: 1, core: 2. Of those that a mesh axis runs over, the one named last changes fastest.
The devices are a block of a 4x4x8 slice.
Arguments:
- left_op: bfloat16 [3072, 3072], P(('batch', 'row'), 'col')
- left_start: float32 [3072, 384], P(('batch', 'row', 'col'))
- right_op: bfloat16 [8192, 8192], P(('batch', 'row'), 'col')
- right_start: float32 [8192, 384], P(('batch', 'row', 'col'))
Outputs:
- output 1: float32 [3072, 384], P(('batch', 'row', 'col'))
- output 2: float32 [384, 384], P('batch')
- output 3: float32 [8192, 384], P(('batch', 'row', 'col'))
- output 4: float32 [384, 384], P('batch')
All inputs are finite; a program needn't handle non-finite values.
Results may differ from the reference program's by a relative error of at most 0.00100245.
Values are sent between devices in bfloat16 or wider.
A program may use at most 768 MiB of HBM per device.

```python
import jax
import jax.numpy as jnp
from jax import lax

N = 3072
N2 = 8192
S = 384
SWEEPS = 4


def build_operator(key, size):
    key_vec, key_val, key_noise = jax.random.split(key, 3)
    eig_basis = jax.random.normal(key_vec, (size, S), jnp.float32) * (size ** -0.5)
    levels = 1.5 * 4.0 ** jax.random.uniform(key_val, (S,), jnp.float32)
    noise_mat = jax.random.normal(key_noise, (size, size), jnp.float32) * (0.1 * size ** -0.5)
    full_mat = jnp.dot(eig_basis * levels, eig_basis.T) + noise_mat
    symmetric = 0.5 * (full_mat + full_mat.T) + 0.5 * jnp.eye(size, dtype=jnp.float32)
    return symmetric.astype(jnp.bfloat16)


def setup_inputs(seed: int = 0, part: int = 0) -> dict:
    base_key = jax.random.fold_in(jax.random.key(seed), part)
    key_left_op, key_left_start, key_right_op, key_right_start = jax.random.split(base_key, 4)
    return {
        "left_op": build_operator(key_left_op, N),
        "left_start": jax.random.normal(key_left_start, (N, S), jnp.float32),
        "right_op": build_operator(key_right_op, N2),
        "right_start": jax.random.normal(key_right_start, (N2, S), jnp.float32),
    }


def cholqr_step(y_mat, gram_mat):
    chol_low = jnp.linalg.cholesky(gram_mat)
    return lax.linalg.triangular_solve(chol_low, y_mat, left_side=False, lower=True, transpose_a=True)


def orthonormalize(y_mat):
    row_count = y_mat.shape[0]
    y_half = y_mat.astype(jnp.bfloat16)
    gram_one = jnp.dot(y_half.T, y_half, preferred_element_type=jnp.float32) / row_count
    y_one = cholqr_step(y_mat, gram_one)
    gram_two = jnp.dot(y_one.T, y_one, precision=lax.Precision.HIGHEST) / row_count
    return cholqr_step(y_one, gram_two)


def iterate(operator, start_block):
    def one_sweep(x_cur, unused):
        y_mat = jnp.dot(operator, x_cur.astype(jnp.bfloat16), preferred_element_type=jnp.float32)
        return orthonormalize(y_mat), None

    x_final, scan_rest = lax.scan(one_sweep, start_block, None, length=SWEEPS)
    z_mat = jnp.dot(operator, x_final.astype(jnp.bfloat16), preferred_element_type=jnp.float32)
    rayleigh = jnp.dot(x_final.T, z_mat, precision=lax.Precision.HIGHEST) / x_final.shape[0]
    return x_final, rayleigh


def reference(left_op, left_start, right_op, right_start):
    left_basis, left_rayleigh = iterate(left_op, left_start)
    right_basis, right_rayleigh = iterate(right_op, right_start)
    return (left_basis, left_rayleigh, right_basis, right_rayleigh)
```

```python
import functools

import jax
import jax.numpy as jnp
from jax import lax
from jax.experimental import pallas as pl
from jax.experimental.pallas import tpu as pltpu
from jax.sharding import PartitionSpec as P

SWEEPS = 4
ROW_CONTRACT = (((0,), (0,)), ((), ()))
LANE_CONTRACT = (((1,), (1,)), ((), ()))

LN=128; PAN=32; SL=8
HI=lax.Precision.HIGHEST
def bl(x, j):
    return jnp.broadcast_to(x[:, j:j+1], (SL, LN))
def bs(x, k):
    return jnp.broadcast_to(x[k:k+1, :], (SL, LN))


def panel(b_ref, w_ref, m, P, nt):
    q = P*PAN//LN
    r0 = P*PAN
    G = PAN//SL
    tB = list(range(q, nt)); tW = list(range(0, q+1))
    B = [[b_ref[m, r0+g*SL:r0+(g+1)*SL, t*LN:(t+1)*LN] for t in tB] for g in range(G)]
    W = [[w_ref[m, r0+g*SL:r0+(g+1)*SL, t*LN:(t+1)*LN] for t in tW] for g in range(G)]
    sub = lax.broadcasted_iota(jnp.int32, (SL, LN), 0)
    gens = []
    for s in range(G):
        c0 = (r0 + s*SL) % LN
        C = [[bl(B[g][0], c0+k) for k in range(SL)] for g in range(s, G)]
        yield
        for k in range(SL):
            p = bs(C[0][k], k)
            rs = lax.rsqrt(p)
            rowB = [bs(x, k)*rs for x in B[s]]
            rowW = [bs(x, k)*rs for x in W[s]]
            crow = {kk: bs(C[0][kk], k)*rs for kk in range(k+1, SL)}
            for gi, g in enumerate(range(s, G)):
                mm = C[gi][k]*rs
                if gi == 0:
                    keep = sub == k
                    mm = jnp.where(sub > k, mm, 0.0)
                    B[g] = [jnp.where(keep, rb, x - mm*rb) for x, rb in zip(B[g], rowB)]
                    W[g] = [jnp.where(keep, rb, x - mm*rb) for x, rb in zip(W[g], rowW)]
                else:
                    B[g] = [x - mm*rb for x, rb in zip(B[g], rowB)]
                    W[g] = [x - mm*rb for x, rb in zip(W[g], rowW)]
                for kk in range(k+1, SL):
                    C[gi][kk] = C[gi][kk] - mm*crow[kk]
            yield
        for i, t in enumerate(tB):
            b_ref[m, r0+s*SL:r0+(s+1)*SL, t*LN:(t+1)*LN] = B[s][i]
        for i, t in enumerate(tW):
            w_ref[m, r0+s*SL:r0+(s+1)*SL, t*LN:(t+1)*LN] = W[s][i]
    yield
    n = nt*LN
    r1 = r0+PAN
    if r1 < n:
        for qq in range(r1//LN, nt):
            lo = max(r1, qq*LN); hi = (qq+1)*LN
            a = b_ref[m, r0:r1, qq*LN:hi]
            at = a.T[lo-qq*LN:, :]
            rhsB = b_ref[m, r0:r1, qq*LN:n]
            b_ref[m, lo:hi, qq*LN:n] = b_ref[m, lo:hi, qq*LN:n] - jnp.dot(at, rhsB, precision=HI, preferred_element_type=jnp.float32)
            rhsW = w_ref[m, r0:r1, 0:(q+1)*LN]
            w_ref[m, lo:hi, 0:(q+1)*LN] = w_ref[m, lo:hi, 0:(q+1)*LN] - jnp.dot(at, rhsW, precision=HI, preferred_element_type=jnp.float32)

def chol_body(scales, g_ref, w_ref, b_ref):
    nm, n, _ = g_ref.shape
    nt = n//LN
    r = lax.broadcasted_iota(jnp.int32, (n, n), 0); c = lax.broadcasted_iota(jnp.int32, (n, n), 1)
    for m in range(nm):
        b_ref[m] = g_ref[m]*scales[m]
        w_ref[m] = jnp.where(r == c, 1.0, 0.0).astype(jnp.float32)
    for pan in range(n//PAN):
        its = [panel(b_ref, w_ref, m, pan, nt) for m in range(nm)]
        done = False
        while not done:
            for it in its:
                try: next(it)
                except StopIteration: done = True

def chol_inv(g, scales):
    nm, n, _ = g.shape
    return pl.pallas_call(functools.partial(chol_body, scales),
        out_shape=jax.ShapeDtypeStruct((nm, n, n), jnp.float32),
        in_specs=[pl.BlockSpec(memory_space=pltpu.VMEM)], out_specs=pl.BlockSpec(memory_space=pltpu.VMEM),
        scratch_shapes=[pltpu.VMEM((nm, n, n), jnp.float32)],
        name="chol_inv")(g)


def gram(lhs_mat, rhs_mat, precision):
    return lax.dot_general(lhs_mat, rhs_mat, ROW_CONTRACT, precision=precision, preferred_element_type=jnp.float32)


def times_rinv(y_mat, l_inv):
    return lax.dot_general(y_mat, l_inv, LANE_CONTRACT, precision=HI, preferred_element_type=jnp.float32)


def solution(mesh):
    row_size = mesh.shape["row"]
    col_size = mesh.shape["col"]
    grid_axes = ("row", "col")
    perm_pairs = [(src_index, (src_index % row_size) * col_size + src_index // row_size) for src_index in range(row_size * col_size)]

    def apply_op(op_blk, x_sub):
        x_moved = lax.ppermute(x_sub.astype(jnp.bfloat16), grid_axes, perm_pairs)
        x_col = lax.all_gather(x_moved, "row", axis=0, tiled=True)
        partial_prod = jnp.dot(op_blk, x_col, preferred_element_type=jnp.float32)
        return lax.psum_scatter(partial_prod, "col", scatter_dimension=0, tiled=True)

    def local_program(left_op, left_start, right_op, right_start):
        scales = (1.0 / (left_op.shape[0] * row_size), 1.0 / (right_op.shape[0] * row_size))

        def normalize(ys, hs, precision):
            grams = lax.psum(jnp.stack([gram(h, h, precision) for h in hs]), grid_axes)
            l_inv = chol_inv(grams, scales)
            return tuple(times_rinv(y, l_inv[i]) for i, y in enumerate(ys))

        def sweep(_, xs):
            ys = (apply_op(left_op, xs[0]), apply_op(right_op, xs[1]))
            ys = normalize(ys, tuple(y.astype(jnp.bfloat16) for y in ys), None)
            return normalize(ys, ys, HI)

        xs = lax.fori_loop(0, SWEEPS, sweep, (left_start, right_start))
        zs = (apply_op(left_op, xs[0]), apply_op(right_op, xs[1]))
        ray = lax.psum(jnp.stack([gram(x, z, HI) for x, z in zip(xs, zs)]), grid_axes)
        return xs[0], ray[0] * scales[0], xs[1], ray[1] * scales[1]

    op_spec = P(("batch", "row"), "col")
    vec_spec = P(("batch", "row", "col"), None)
    small_spec = P("batch", None)
    return jax.shard_map(local_program, mesh=mesh, in_specs=(op_spec, vec_spec, op_spec, vec_spec), out_specs=(vec_spec, small_spec, vec_spec, small_spec), check_vma=False)
```

```python
import functools

import jax
import jax.numpy as jnp
from jax import lax
from jax.experimental import pallas as pl
from jax.experimental.pallas import tpu as pltpu
from jax.sharding import PartitionSpec as P

SWEEPS = 4
GRAIN = 512
LN=128; PAN=32; SL=8
HI=lax.Precision.HIGHEST

def bl(x, j):
    return jnp.broadcast_to(x[:, j:j+1], (SL, LN))

def bs(x, k):
    return jnp.broadcast_to(x[k:k+1, :], (SL, LN))


def panel(b_ref, w_ref, m, P, nt):
    q = P*PAN//LN
    r0 = P*PAN
    G = PAN//SL
    tB = list(range(q, nt)); tW = list(range(0, q+1))
    B = [[b_ref[m, r0+g*SL:r0+(g+1)*SL, t*LN:(t+1)*LN] for t in tB] for g in range(G)]
    W = [[w_ref[m, r0+g*SL:r0+(g+1)*SL, t*LN:(t+1)*LN] for t in tW] for g in range(G)]
    sub = lax.broadcasted_iota(jnp.int32, (SL, LN), 0)
    gens = []
    for s in range(G):
        c0 = (r0 + s*SL) % LN
        C = [[bl(B[g][0], c0+k) for k in range(SL)] for g in range(s, G)]
        yield
        for k in range(SL):
            p = bs(C[0][k], k)
            rs = lax.rsqrt(p)
            rowB = [bs(x, k)*rs for x in B[s]]
            rowW = [bs(x, k)*rs for x in W[s]]
            crow = {kk: bs(C[0][kk], k)*rs for kk in range(k+1, SL)}
            for gi, g in enumerate(range(s, G)):
                mm = C[gi][k]*rs
                if gi == 0:
                    keep = sub == k
                    mm = jnp.where(sub > k, mm, 0.0)
                    B[g] = [jnp.where(keep, rb, x - mm*rb) for x, rb in zip(B[g], rowB)]
                    W[g] = [jnp.where(keep, rb, x - mm*rb) for x, rb in zip(W[g], rowW)]
                else:
                    B[g] = [x - mm*rb for x, rb in zip(B[g], rowB)]
                    W[g] = [x - mm*rb for x, rb in zip(W[g], rowW)]
                for kk in range(k+1, SL):
                    C[gi][kk] = C[gi][kk] - mm*crow[kk]
            yield
        for i, t in enumerate(tB):
            b_ref[m, r0+s*SL:r0+(s+1)*SL, t*LN:(t+1)*LN] = B[s][i]
        for i, t in enumerate(tW):
            w_ref[m, r0+s*SL:r0+(s+1)*SL, t*LN:(t+1)*LN] = W[s][i]
    yield
    n = nt*LN
    r1 = r0+PAN
    if r1 < n:
        for qq in range(r1//LN, nt):
            lo = max(r1, qq*LN); hi = (qq+1)*LN
            a = b_ref[m, r0:r1, qq*LN:hi]
            at = a.T[lo-qq*LN:, :]
            rhsB = b_ref[m, r0:r1, qq*LN:n]
            b_ref[m, lo:hi, qq*LN:n] = b_ref[m, lo:hi, qq*LN:n] - jnp.dot(at, rhsB, precision=HI, preferred_element_type=jnp.float32)
            rhsW = w_ref[m, r0:r1, 0:(q+1)*LN]
            w_ref[m, lo:hi, 0:(q+1)*LN] = w_ref[m, lo:hi, 0:(q+1)*LN] - jnp.dot(at, rhsW, precision=HI, preferred_element_type=jnp.float32)

MESH = pl.DeviceIdType.MESH
RING = 4


def where_am_i():
    row = lax.axis_index("row")
    col = lax.axis_index("col")
    return row, col // 2, col % 2


def rows_at(start, size):
    return pl.ds(pl.multiple_of(start, 8), size)


class Links:
    def __init__(self, send, recv):
        self.send, self.recv, self.used = send, recv, 0
        self.row, self.col_x, self.core = where_am_i()
        self.open = []
    def pos(self, axis):
        return self.row if axis == "y" else self.col_x
    def peer(self, axis, step):
        if axis == "core":
            return {"row": self.row, "col": self.col_x * 2 + (1 - self.core)}
        if axis == "y":
            return {"row": (self.row + step) % RING, "col": self.col_x * 2 + self.core}
        return {"row": self.row, "col": ((self.col_x + step) % RING) * 2 + self.core}
    def copy(self, src, dst, axis, step=0):
        slot = self.used
        self.used += 1
        desc = pltpu.make_async_remote_copy(src_ref=src, dst_ref=dst, send_sem=self.send.at[slot], recv_sem=self.recv.at[slot], device_id=self.peer(axis, step), device_id_type=MESH)
        desc.start()
        self.open.append(desc)
        return desc
    def greet(self, who):
        barrier = pltpu.get_barrier_semaphore()
        for axis, step in who:
            pl.semaphore_signal(barrier, inc=1, device_id=self.peer(axis, step), device_id_type=MESH)
        pl.semaphore_wait(barrier, len(who))
    def drain(self):
        for desc in self.open:
            desc.wait_send()


def total_kernel(g_ref, out_ref, r_a, acc, r_b, part, r_c, fin, send, recv):
    rows = g_ref.shape[0]
    half, quart = rows // 2, rows // 4
    big, small = quart // RING, quart // RING // RING
    net = Links(send, recv)
    core = net.core
    net.greet([("core", 0)] + [(a, s) for a in ("x", "y") for s in (1, 2, 3)])
    first, second = ("x", "y"), ("y", "x")
    steps = (2, 1, 3, 0)
    swap = {}
    for s in steps:
        for h in range(2):
            j = (net.pos(first[h]) + s) % RING
            off = h * quart + j * big
            swap[h, s] = net.copy(g_ref.at[rows_at((1 - core) * half + off, big)], r_a.at[rows_at(off, big)], "core")
    out_b = {}
    for s in steps:
        for h in range(2):
            j = (net.pos(first[h]) + s) % RING
            off = h * quart + j * big
            swap[h, s].wait_recv()
            acc[rows_at(off, big)] = g_ref[rows_at(core * half + off, big)] + r_a[rows_at(off, big)]
            if s:
                out_b[h, s] = net.copy(acc.at[rows_at(off, big)], r_b.at[h, s - 1], first[h], s)
    for h in range(2):
        tot = acc[rows_at(h * quart + net.pos(first[h]) * big, big)]
        for s in (1, 3, 2):
            out_b[h, s].wait_recv()
            tot = tot + r_b[h, s - 1]
        part[h] = tot
    out_c = {}
    for s in (2, 1, 3):
        for h in range(2):
            j = (net.pos(second[h]) + s) % RING
            out_c[h, s] = net.copy(part.at[h, rows_at(j * small, small)], r_c.at[h, s - 1], second[h], s)
    base = [core * half + h * quart + net.pos(first[h]) * big for h in range(2)]
    out_d = {}
    for h in range(2):
        mine = net.pos(second[h]) * small
        tot = part[h, rows_at(mine, small)]
        for s in (1, 3, 2):
            out_c[h, s].wait_recv()
            tot = tot + r_c[h, s - 1]
        fin[rows_at(base[h] + mine, small)] = tot
        at = rows_at(base[h] + mine, small)
        for s in (2, 1, 3):
            out_d[h, s] = net.copy(fin.at[at], fin.at[at], second[h], s)
    out_e, out_f = {}, []
    for h in range(2):
        for s in (1, 3, 2):
            out_d[h, s].wait_recv()
        at = rows_at(base[h], big)
        for s in (2, 1, 3):
            out_e[h, s] = net.copy(fin.at[at], fin.at[at], first[h], s)
        out_f.append(net.copy(fin.at[at], fin.at[at], "core"))
    for s in (1, 3, 2):
        for h in range(2):
            out_e[h, s].wait_recv()
            j = (net.pos(first[h]) + RING - s) % RING
            at = rows_at(core * half + h * quart + j * big, big)
            out_f.append(net.copy(fin.at[at], fin.at[at], "core"))
    for desc in out_f:
        desc.wait_recv()
    net.drain()
    out_ref[...] = fin[...]


def grid_total(g, collective_id):
    rows = g.shape[0]
    big = rows // 16
    n_copies = 8 + 6 + 6 + 6 + 6 + 8
    f32 = jnp.float32
    vm = pl.BlockSpec(memory_space=pltpu.VMEM)
    return pl.pallas_call(total_kernel, out_shape=jax.ShapeDtypeStruct(g.shape, f32), in_specs=[vm], out_specs=vm,
        scratch_shapes=[pltpu.VMEM((rows // 2, 128), f32), pltpu.VMEM((rows // 2, 128), f32), pltpu.VMEM((2, 3, big, 128), f32), pltpu.VMEM((2, big, 128), f32), pltpu.VMEM((2, 3, big // 4, 128), f32), pltpu.VMEM((rows, 128), f32),
            pltpu.SemaphoreType.DMA((n_copies,)), pltpu.SemaphoreType.DMA((n_copies,))],
        compiler_params=pltpu.CompilerParams(collective_id=collective_id, has_side_effects=True), name="grid_total")(g)

COL_PAIR = 2
TRI = ((0, 0), (0, 1), (0, 2), (1, 1), (1, 2), (2, 2))


class Product:
    def __init__(self, net, across, op, x, y, xg, prod, pair, relay, final):
        self.net, self.across = net, across
        self.op, self.x, self.y, self.xg, self.prod, self.pair, self.relay, self.final = op, x, y, xg, prod, pair, relay, final
        self.gat, self.red = ("y", "x") if across else ("x", "y")
        self.sub = x.shape[0]
        self.gpos, self.rpos = net.pos(self.gat), net.pos(self.red)

    def xrow(self, pos, core=None):
        core = self.net.core if core is None else core
        return pos * self.sub if self.across else (pos * COL_PAIR + core) * self.sub

    def at(self, pos, lo=0, size=None, core=None):
        return self.xg.at[rows_at(self.xrow(pos, core) + lo, self.sub if size is None else size)]

    def near(self, step):
        return (self.gpos + step) % RING

    def s0(self):
        own = self.at(self.gpos)
        self.to_r = self.net.copy(self.x, own, self.gat, 1)
        self.to_l = self.net.copy(self.x, own, self.gat, 3)
        self.cores = []
        if not self.across:
            self.cores.append(self.net.copy(self.x, own, "core"))
        self.xg[rows_at(self.xrow(self.gpos), self.sub), :] = self.x[...]

    def s1(self):
        hs = self.sub // 2
        self.to_r.wait_recv()
        ref = self.at(self.near(3), 0, hs)
        self.fw_r = self.net.copy(ref, ref, self.gat, 1)
        self.to_l.wait_recv()
        ref = self.at(self.near(1), hs, hs)
        self.fw_l = self.net.copy(ref, ref, self.gat, 3)
        if not self.across:
            for step in (3, 1):
                ref = self.at(self.near(step))
                self.cores.append(self.net.copy(ref, ref, "core"))

    def s2(self):
        hs = self.sub // 2
        self.fw_r.wait_recv()
        self.fw_l.wait_recv()
        if not self.across:
            ref = self.at(self.near(2))
            self.cores.append(self.net.copy(ref, ref, "core"))
            for desc in self.cores:
                desc.wait_recv()

    def chunk_row(self, step, core=None):
        pos = (self.rpos + step) % RING
        core = self.net.core if core is None else core
        return (pos * COL_PAIR + core) * self.sub if self.across else pos * self.sub

    def multiply(self, start):
        at = rows_at(start, self.sub)
        self.prod[at, :] = jnp.dot(self.op[at, :], self.xg[...], preferred_element_type=jnp.float32)

    def chunk(self, step, slot):
        if self.across:
            other = self.chunk_row(step, 1 - self.net.core)
            self.multiply(other)
            desc = self.net.copy(self.prod.at[rows_at(other, self.sub)], self.pair.at[slot], "core")
            mine = self.chunk_row(step)
            self.multiply(mine)
            return desc
        self.multiply(self.chunk_row(step))

    def settle(self, step, slot, desc):
        if desc is not None:
            desc.wait_recv()
            at = rows_at(self.chunk_row(step), self.sub)
            self.prod[at, :] = self.prod[at, :] + self.pair[slot]

    def half(self, step, h):
        return rows_at(self.chunk_row(step) + h * (self.sub // 2), self.sub // 2)

    def s3(self):
        self.p2 = self.chunk(2, 0)
        if self.across:
            self.p1 = self.chunk(1, 1)
        self.settle(2, 0, self.p2)
        self.rel_r = self.net.copy(self.prod.at[self.half(2, 0)], self.relay.at[0], self.red, 1)
        self.rel_l = self.net.copy(self.prod.at[self.half(2, 1)], self.relay.at[1], self.red, 3)

    def s4(self):
        hs = self.sub // 2
        if not self.across:
            self.p1 = self.chunk(1, 1)
        self.p3 = self.chunk(3, 2)
        self.settle(1, 1, self.p1)
        self.dir_r = self.net.copy(self.prod.at[self.half(1, 1)], self.final.at[0, hs:, :], self.red, 1)
        self.p0 = self.chunk(0, 3)
        self.settle(3, 2, self.p3)
        self.dir_l = self.net.copy(self.prod.at[self.half(3, 0)], self.final.at[1, :hs, :], self.red, 3)

    def s5(self):
        hs = self.sub // 2
        self.rel_r.wait_recv()
        at = self.half(1, 0)
        self.prod[at, :] = self.prod[at, :] + self.relay[0]
        self.sum_r = self.net.copy(self.prod.at[at], self.final.at[0, :hs, :], self.red, 1)
        self.rel_l.wait_recv()
        at = self.half(3, 1)
        self.prod[at, :] = self.prod[at, :] + self.relay[1]
        self.sum_l = self.net.copy(self.prod.at[at], self.final.at[1, hs:, :], self.red, 3)

    def s6(self):
        self.settle(0, 3, self.p0)
        for desc in (self.dir_r, self.dir_l, self.sum_r, self.sum_l):
            desc.wait_recv()
        self.y[...] = self.prod[rows_at(self.chunk_row(0), self.sub), :] + self.final[0] + self.final[1]


def apply_kernel(left_across, lop, lx, rop, rx, ly, ry, g_ref, lxg, lprod, lpair, lrelay, lfinal, rxg, rprod, rpair, rrelay, rfinal, send, recv):
    net = Links(send, recv)
    net.greet([("core", 0)] + [(a, s) for a in ("x", "y") for s in (1, 3)])
    right = Product(net, not left_across, rop, rx, ry, rxg, rprod, rpair, rrelay, rfinal)
    left = Product(net, left_across, lop, lx, ly, lxg, lprod, lpair, lrelay, lfinal)
    for stage in range(7):
        getattr(right, f"s{stage}")()
        getattr(left, f"s{stage}")()
    net.drain()
    for i, y in enumerate((ly, ry)):
        h = y[...].astype(jnp.bfloat16)
        for j, (a, b) in enumerate(TRI):
            g_ref[(i*6+j)*128:(i*6+j+1)*128, :] = lax.dot_general(h[:, a*128:(a+1)*128], h[:, b*128:(b+1)*128], (((0,), (0,)), ((), ())), preferred_element_type=jnp.float32)


def apply_pair(left_across, lop, lx, rop, rx, collective_id):
    f32, bf = jnp.float32, jnp.bfloat16
    s = lx.shape[1]
    vm = pl.BlockSpec(memory_space=pltpu.VMEM)
    scratch = []
    for op, x in ((lop, lx), (rop, rx)):
        sub = x.shape[0]
        scratch += [pltpu.VMEM((op.shape[1], s), bf), pltpu.VMEM((op.shape[0], s), f32), pltpu.VMEM((4, sub, s), f32), pltpu.VMEM((2, sub//2, s), f32), pltpu.VMEM((2, sub, s), f32)]
    n = 2*(2+2+6) + 4 + 4
    scratch += [pltpu.SemaphoreType.DMA((n,)), pltpu.SemaphoreType.DMA((n,))]
    return pl.pallas_call(functools.partial(apply_kernel, left_across),
        out_shape=(jax.ShapeDtypeStruct(lx.shape, f32), jax.ShapeDtypeStruct(rx.shape, f32), jax.ShapeDtypeStruct((12*128, 128), f32)),
        in_specs=[vm]*4, out_specs=(vm,)*3, scratch_shapes=scratch,
        compiler_params=pltpu.CompilerParams(collective_id=collective_id, has_side_effects=True, vmem_limit_bytes=48*1024*1024), name="apply_%s" % ("n" if left_across else "t"))(lop, lx, rop, rx)

ROW_CONTRACT = (((0,), (0,)), ((), ()))
LANE_CONTRACT = (((1,), (1,)), ((), ()))


def orth_kernel(last, scales, g_ref, ly, ry, lo, ro, extra_l, extra_r, w_ref, b_ref):
    nm, n, _ = w_ref.shape
    nt = n // LN
    r = lax.broadcasted_iota(jnp.int32, (n, n), 0)
    c = lax.broadcasted_iota(jnp.int32, (n, n), 1)
    for m in range(nm):
        for j, (a, b) in enumerate(TRI):
            at = (m * len(TRI) + j) * LN
            b_ref[m, a * LN:(a + 1) * LN, b * LN:(b + 1) * LN] = g_ref[at:at + LN, :] * scales[m]
        w_ref[m] = jnp.where(r == c, 1.0, 0.0).astype(jnp.float32)
    for pan in range(n // PAN):
        its = [panel(b_ref, w_ref, m, pan, nt) for m in range(nm)]
        done = False
        while not done:
            for it in its:
                try:
                    next(it)
                except StopIteration:
                    done = True
    for m, (y, o) in enumerate(((ly, lo), (ry, ro))):
        x = lax.dot_general(y[...], w_ref[m], LANE_CONTRACT, precision=HI, preferred_element_type=jnp.float32)
        o[...] = x
        if last:
            (extra_l, extra_r)[m][...] = x.astype(jnp.bfloat16)
        else:
            for j, (a, b) in enumerate(TRI):
                at = (m * len(TRI) + j) * LN
                extra_l[at:at + LN, :] = lax.dot_general(x[:, a * LN:(a + 1) * LN], x[:, b * LN:(b + 1) * LN], ROW_CONTRACT, precision=HI, preferred_element_type=jnp.float32)


def orth_first(scales, g_ref, ly, ry, lo, ro, g2, w_ref, b_ref):
    orth_kernel(False, scales, g_ref, ly, ry, lo, ro, g2, None, w_ref, b_ref)


def orth_second(scales, g_ref, ly, ry, lo, ro, lh, rh, w_ref, b_ref):
    orth_kernel(True, scales, g_ref, ly, ry, lo, ro, lh, rh, w_ref, b_ref)


def orth(last, scales, g, ly, ry):
    n = ly.shape[1]
    f32, bf = jnp.float32, jnp.bfloat16
    vm = pl.BlockSpec(memory_space=pltpu.VMEM)
    like = lambda v, t: jax.ShapeDtypeStruct(v.shape, t)
    extra = (like(ly, bf), like(ry, bf)) if last else (like(g, f32),)
    return pl.pallas_call(functools.partial(orth_second if last else orth_first, scales),
        out_shape=(like(ly, f32), like(ry, f32)) + extra,
        in_specs=[vm] * 3, out_specs=(vm,) * (2 + len(extra)),
        scratch_shapes=[pltpu.VMEM((2, n, n), f32), pltpu.VMEM((2, n, n), f32)],
        name="orth_second" if last else "orth_first")(g, ly, ry)


def solution(mesh):
    row_size = mesh.shape["row"]
    col_size = mesh.shape["col"]
    grid_axes = ("row", "col")
    to_cols = [(i, (i % row_size) * col_size + i // row_size) for i in range(row_size * col_size)]
    to_rows = [(b, a) for a, b in to_cols]

    def local_program(left_op, left_start, right_op, right_start):
        scales = (1.0 / (left_op.shape[0] * row_size), 1.0 / (right_op.shape[0] * row_size))
        left_t, right_t = left_op.T, right_op.T

        def normalize(ys, g):
            ly, ry, g2 = orth(False, scales, grid_total(g, 2), ys[0], ys[1])
            return orth(True, scales, grid_total(g2, 2), ly, ry)

        def two_sweeps(_, carry):
            lh, rh = carry[2:]
            ly, ry, g = apply_pair(True, left_op, lh, right_t, rh, 0)
            _, _, lh, rh = normalize((ly, ry), g)
            ly, ry, g = apply_pair(False, left_t, lh, right_op, rh, 1)
            return normalize((ly, ry), g)

        lh = lax.ppermute(left_start.astype(jnp.bfloat16), grid_axes, to_cols)
        carry = (left_start, right_start, lh, right_start.astype(jnp.bfloat16))
        lx_cols, rx, lh, rh = lax.fori_loop(0, SWEEPS // 2, two_sweeps, carry)
        lx = lax.ppermute(lx_cols, grid_axes, to_rows)
        rx_cols = lax.ppermute(rx, grid_axes, to_cols)
        lz, rz_cols, _ = apply_pair(True, left_op, lh, right_t, rh, 0)
        n = lx.shape[1]
        parts = []
        for x, z in ((lx, lz), (rx_cols, rz_cols)):
            for t in range(n // LN):
                parts.append(lax.dot_general(x, z[:, t * LN:(t + 1) * LN], ROW_CONTRACT, precision=HI, preferred_element_type=jnp.float32))
        rows = sum(part.shape[0] for part in parts)
        parts.append(jnp.zeros((-rows % GRAIN, LN), jnp.float32))
        ray = grid_total(jnp.concatenate(parts, axis=0), 3)[:rows]
        ray = ray.reshape(2, n // LN, n, LN).transpose(0, 2, 1, 3).reshape(2, n, n)
        return lx, ray[0] * scales[0], rx, ray[1] * scales[1]

    op_spec = P(("batch", "row"), "col")
    vec_spec = P(("batch", "row", "col"), None)
    small_spec = P("batch", None)
    return jax.shard_map(local_program, mesh=mesh, in_specs=(op_spec, vec_spec, op_spec, vec_spec), out_specs=(vec_spec, small_spec, vec_spec, small_spec), check_vma=False)
```
